32 devices in a mesh: bank: 4 (over x, core), zero: 8 (over z, y).
Axes of the slice: x: 2, y: 2, z: 4, core: 2. Of those that a mesh axis runs over, the one named last changes fastest.
Arguments:
- w_gate: float32 [64, 2048, 1024], P('bank', 'zero'), may hold values from -0.1875 to 0.1875
- avg_gate: float32 [64, 2048, 1024], P('bank', 'zero'), may hold values from -0.125 to 0.125
- w_up: float32 [64, 2048, 1024], P('bank', 'zero'), may hold values from -0.1875 to 0.1875
- avg_up: float32 [64, 2048, 1024], P('bank', 'zero'), may hold values from -0.125 to 0.125
- mix_share: float32 [64], P('bank'), may hold values from 0.2 to 0.8
- router_weight: float32 [2048, 64], P('zero', 'bank'), may hold values from -0.125 to 0.125
- router_gain: float32 [2048], P('zero'), may hold values from 0.25 to 1.75
Outputs:
- serve_gate: bfloat16 [64, 2048, 1024], P('bank', None, 'zero')
- serve_up: bfloat16 [64, 2048, 1024], P('bank', None, 'zero')
- scale_gate: float32 [64, 1024], P('bank', 'zero')
- scale_up: float32 [64, 1024], P('bank', 'zero')
- serve_router: bfloat16 [2048, 64], replicated
The draws below stay inside these ranges and needn't reach their ends.
All inputs are finite; a program needn't handle non-finite values. Where the reference program divides by a largest or mean magnitude, that divisor is 1e-20 or more.
Results may differ from the reference program's by a relative error of at most 0.001.
Values may be sent and summed in bfloat16 or wider, within the bound.
A program may use at most 256 MiB of HBM per device.

```python
import jax
import jax.numpy as jnp

EXPERTS = 64
D_MODEL = 2048
D_EXPERT = 1024


def strengthened(drawn, key, source, target, parts, factor):
    def block_of(position):
        return (jnp.arange(drawn.shape[position]) // (drawn.shape[position] // parts)).reshape((-1,) + (1,) * (drawn.ndim - 1 - position))

    near = jax.random.permutation(key, parts)[block_of(target)]
    second = (block_of(target) + parts // 2) % parts
    return jnp.where((block_of(source) == near) | (block_of(source) == second), factor * drawn, drawn)


def levels(rng, dims, shards, smallest, largest):
    def one(axis_at, blocks):
        steps = jax.random.uniform(jax.random.fold_in(jax.random.fold_in(rng, 6), axis_at), (blocks,), jnp.float32, smallest / len(shards), largest / len(shards))
        return jnp.repeat(jnp.exp(steps), dims[axis_at] // blocks).reshape((-1,) + (1,) * (len(dims) - axis_at - 1))

    factor_of = one(*shards[0])
    for cut in shards[1:]:
        factor_of = factor_of * one(*cut)
    return factor_of


def gaussian(key, dims, deviation, most, pieces=(), kind=jnp.bfloat16):
    array = jax.random.normal(key, dims, jnp.float32) * deviation
    if len(pieces) > 0:
        array = levels(key, dims, pieces, -0.22, 0.18) * array
    return jnp.clip(array, min=-most, max=most).astype(kind)


def heavy_noise(stream_key, extent, scale, bound, pieces, heavy, held_as=jnp.bfloat16):
    array = scale * jax.random.normal(stream_key, extent, jnp.float32)
    if pieces:
        array = array * levels(stream_key, extent, pieces, -0.22, 0.18)
    return jnp.clip(strengthened(array, jax.random.fold_in(stream_key, 3), *heavy), -bound, bound).astype(held_as)


def setup_inputs(seed: int = 0) -> dict:
    arg_keys = jax.random.split(jax.random.key(seed), 8)
    w_gate = heavy_noise(arg_keys[0], (EXPERTS, D_MODEL, D_EXPERT), D_MODEL ** -0.5, 0.1875, ((0, 4), (1, 8)), (1, 2, 8, 2.0), jnp.float32)
    avg_gate = gaussian(arg_keys[1], (EXPERTS, D_MODEL, D_EXPERT), D_MODEL ** -0.5, 0.125, ((0, 4), (1, 8)), jnp.float32)
    w_up = heavy_noise(arg_keys[2], (EXPERTS, D_MODEL, D_EXPERT), D_MODEL ** -0.5, 0.1875, ((0, 4), (1, 8)), (1, 2, 8, 2.0), jnp.float32)
    avg_up = gaussian(arg_keys[3], (EXPERTS, D_MODEL, D_EXPERT), D_MODEL ** -0.5, 0.125, ((0, 4), (1, 8)), jnp.float32)
    mix_share = jnp.clip(0.2 + 0.6 * jax.random.uniform(arg_keys[4], (EXPERTS,), jnp.float32) ** levels(arg_keys[4], (EXPERTS,), ((0, 4),), -0.2, 0.2), 0.2, 0.8)
    router_weight = gaussian(arg_keys[5], (D_MODEL, EXPERTS), D_MODEL ** -0.5, 0.125, ((0, 8), (1, 4)), jnp.float32)
    router_gain = jnp.clip(1.0 + 0.15 * jax.random.normal(arg_keys[6], (D_MODEL,), jnp.float32), 0.25, 1.75)
    return {"w_gate": w_gate, "avg_gate": avg_gate, "w_up": w_up, "avg_up": avg_up, "mix_share": mix_share, "router_weight": router_weight, "router_gain": router_gain}


def reference(w_gate, avg_gate, w_up, avg_up, mix_share, router_weight, router_gain):
    fresh_gate = mix_share[:, None, None] * w_gate + (1.0 - mix_share[:, None, None]) * avg_gate
    fresh_up = mix_share[:, None, None] * w_up + (1.0 - mix_share[:, None, None]) * avg_up
    scale_gate = jnp.sum(jnp.abs(fresh_gate), axis=1) / D_MODEL
    serve_gate = (fresh_gate / jnp.expand_dims(scale_gate, 1)).astype(jnp.bfloat16)
    scale_up = jnp.sum(jnp.abs(fresh_up), axis=1) / D_MODEL
    serve_up = (fresh_up / jnp.expand_dims(scale_up, 1)).astype(jnp.bfloat16)
    serve_router = (router_weight * router_gain[:, None]).astype(jnp.bfloat16)
    return serve_gate, serve_up, scale_gate, scale_up, serve_router
```

```python
import functools

import jax
import jax.numpy as jnp
from jax import lax
from jax.experimental import pallas as pl
from jax.experimental.pallas import tpu as pltpu
from jax.sharding import PartitionSpec as P

MESH = pl.DeviceIdType.MESH
HEAD = 3
RING = 2
STEP = 32


def partner(me, k, n):
    out, bit = me, 1
    while bit < n:
        if k & bit:
            out = out + bit * (1 - 2 * ((me // bit) % 2))
        bit *= 2
    return out


def kernel(
    nz, nb, head,
    mix_in, wg, ag, wu, au, rw_in, gain_in,
    land, scl, rt,
    mix, rw, gain, stage, send, pa, ra, sa, part, rs, half, other, sb, rtp,
    small_sem, in_sem, pa_ssem, pa_rsem, step_ssem, step_rsem, bulk_ssem, bulk_rsem, r_ssem, r_rsem,
):
    me = lax.axis_index("zero")
    bank = lax.axis_index("bank")
    experts, rows, _ = wg.shape
    cb = land.shape[3]
    eb = rw.shape[0]
    tail = experts - head
    nh = nz // 2
    near = lax.rem(me, nh)
    ws, avgs = (wg, wu), (ag, au)
    peers = [partner(me, k, nz) for k in range(1, nz)]
    inner, far = peers[:nh - 1], peers[nh - 1]
    banks = [partner(bank, k, nb) for k in range(1, nb)]

    def loads(e, slot):
        for m in range(2):
            for i, source in enumerate((ws[m], avgs[m])):
                pltpu.make_async_copy(source.at[e], stage.at[slot, m, i], in_sem.at[slot]).start()

    def loaded(slot):
        pltpu.make_async_copy(stage.at[slot], stage.at[slot], in_sem.at[slot]).wait()

    def to(p, source, target, ssem, rsem):
        pltpu.make_async_remote_copy(
            source, target, ssem, rsem, device_id={"zero": p}, device_id_type=MESH).start()

    def sent(ref, sem):
        pltpu.make_async_copy(ref, ref, sem).wait()

    small = [
        pltpu.make_async_copy(mix_in, mix, small_sem.at[0]),
        pltpu.make_async_copy(rw_in, rw, small_sem.at[1]),
        pltpu.make_async_copy(gain_in, gain, small_sem.at[2]),
    ]
    small[0].start()
    for e in range(head):
        loads(e, e)

    barrier = pltpu.get_barrier_semaphore()
    for p in peers:
        pl.semaphore_signal(barrier, inc=1, device_id={"zero": p}, device_id_type=MESH)
    for p in banks:
        pl.semaphore_signal(barrier, inc=1, device_id={"bank": p}, device_id_type=MESH)
    for c in small[1:]:
        c.start()

    def ring(i):
        return head + lax.rem(i, RING)

    def fresh(slot, e, m, d, span):
        cols = slice(d * cb, (d + 1) * cb)
        a = mix[e]
        return a * stage[slot, m, 0, span, cols] + (1.0 - a) * stage[slot, m, 1, span, cols]

    def sizes_of(slot, e, m):
        def body(i, sums):
            span = pl.ds(pl.multiple_of(i * STEP, STEP), STEP)
            out = []
            for d in range(nz):
                v = jnp.abs(fresh(slot, e, m, d, span))
                out.append(sums[d] + sum(v[j:j + 8] for j in range(0, STEP, 8)))
            return tuple(out)

        sums = lax.fori_loop(0, rows // STEP, body, tuple(jnp.zeros((8, cb), jnp.float32) for _ in range(nz)))
        return [jnp.sum(s, axis=0, keepdims=True) for s in sums]

    def head_sizes(e):
        loaded(e)
        for m in range(2):
            for d, size in enumerate(sizes_of(e, e, m)):
                pa[e, m, d:d + 1, :] = size

    def head_send(e):
        for k, p in enumerate(peers):
            to(p, pa.at[e], ra.at[e, k], pa_ssem.at[e], pa_rsem.at[e])

    def head_scale(e):
        sent(ra.at[e], pa_rsem.at[e])
        total = pa[e]
        for k in range(nz - 1):
            total = total + ra[e, k]
        sa[e] = total / (rows * nz)
        for m in range(2):
            scl[m, e:e + 1, :] = sa[e, m, pl.ds(me, 1), :]

    place = pl.ds(pl.multiple_of(me * rows, rows), rows)

    def narrow(slot, e, m, scale):
        inverses = [1.0 / scale(m, d) for d in range(nz)]

        def body(i, carry):
            span = pl.ds(pl.multiple_of(i * STEP, STEP), STEP)
            for d in range(nz):
                send[m, d, e, span, :] = (fresh(slot, e, m, d, span) * inverses[d]).astype(send.dtype)
            return carry

        lax.fori_loop(0, rows // STEP, body, 0)

    def push(e, m):
        land[m, e, place, :] = send[m, me, e]
        for p in peers:
            to(p, send.at[m, p, e], land.at[m, e, place], bulk_ssem, bulk_rsem)

    def tail_sizes(i, carry):
        e = head + i
        loaded(ring(i))
        for m in range(2):
            for d, size in enumerate(sizes_of(ring(i), e, m)):
                part[d // nh, d % nh, pl.ds(m * tail + i, 1), :] = size

        @pl.when(i + RING < tail)
        def _():
            loads(e + RING, ring(i))

        return carry

    small[0].wait()
    head_sizes(0)
    for i in range(min(RING, tail)):
        loads(head + i, ring(i))
    pl.semaphore_wait(barrier, nz - 1 + nb - 1)
    head_send(0)
    for c in small[1:]:
        c.wait()
    rtp[...] = (rw[...] * gain[...]).astype(rtp.dtype)
    band = pl.ds(pl.multiple_of(bank * eb, eb), eb)
    flat = len(rt.shape) == 2
    if flat:
        mine = rt.at[band, place]
        theirs = rt.at[band, pl.ds(pl.multiple_of(far * rows, rows), rows)]
        tiles = rt.at[band, pl.ds(0, 2 * (nh - 1) * rows)]
        column = rt.at[band]
        others = rt.at[pl.ds(0, (nb - 1) * eb)]
        rt[band, place] = rtp[...]
    else:
        mine = rt.at[me, band]
        theirs = rt.at[far, band]
        tiles = rt.at[pl.ds(0, 2 * (nh - 1)), band]
        column = rt.at[:, band]
        others = rt.at[:, pl.ds(0, (nb - 1) * eb)]
        rt[me, band] = rtp[...]
    to(far, rtp, mine, r_ssem.at[0], r_rsem.at[0])
    for e in range(1, head):
        head_sizes(e)
        head_send(e)
    part[:, :, 2 * tail:, :] = jnp.zeros_like(part[:, :, 2 * tail:, :])

    for e in range(head):
        head_scale(e)
        for m in range(2):
            narrow(e, e, m, lambda m, d, e=e: sa[e, m, d:d + 1, :])
            if e == 0:
                push(e, m)
    lax.fori_loop(0, tail, tail_sizes, 0)

    for k, p in enumerate(inner):
        to(p, part.at[:, lax.rem(p, nh)], rs.at[k], step_ssem.at[0], step_rsem.at[0])
    push(1, 0)
    for i in range(min(RING, tail)):
        loads(head + i, ring(i))
    pltpu.make_async_copy(theirs, theirs, r_rsem.at[0]).wait()
    for p in inner:
        for tile in (mine, theirs):
            to(p, tile, tile, r_ssem.at[1], r_rsem.at[1])

    sent(rs, step_rsem.at[0])
    total = part[:, near]
    for k in range(nh - 1):
        total = total + rs[k]
    half[...] = total
    to(far, half, other, step_ssem.at[1], step_rsem.at[1])
    push(1, 1)

    sent(other, step_rsem.at[1])
    total = (half[...] + other[...]) / (rows * nz)
    sb[:, near] = total
    for m in range(2):
        scl[m, head:, :] = sb[me // nh, near, m * tail:(m + 1) * tail, :]
    for p in inner:
        to(p, sb.at[:, near], sb.at[:, near], step_ssem.at[2], step_rsem.at[2])
    for e in range(2, head):
        for m in range(2):
            push(e, m)

    sent(tiles, r_rsem.at[1])
    for p in banks:
        pltpu.make_async_remote_copy(
            column, column, r_ssem.at[2], r_rsem.at[2], device_id={"bank": p}, device_id_type=MESH).start()
    sent(rs, step_rsem.at[2])

    def serve(i, carry):
        e = head + i
        loaded(ring(i))
        for m in range(2):
            narrow(ring(i), e, m, lambda m, d: sb[d // nh, d % nh, pl.ds(m * tail + i, 1), :])
            push(e, m)

        @pl.when(i + RING < tail)
        def _():
            loads(e + RING, ring(i))

        return carry

    lax.fori_loop(0, tail, serve, 0)

    for e in range(head):
        sent(ra.at[e], pa_ssem.at[e])
    sent(rs, step_ssem.at[0])
    sent(other, step_ssem.at[1])
    sent(rs, step_ssem.at[2])
    sent(rtp, r_ssem.at[0])
    sent(tiles, r_ssem.at[1])
    for sem in (r_ssem, r_rsem):
        sent(others, sem.at[2])
    sent(send.at[:, pl.ds(0, nz - 1)], bulk_ssem)
    sent(land.at[:, :, pl.ds(0, (nz - 1) * rows)], bulk_rsem)


def settle(land, scl, rt, og, ou, sg, su, out, sem):
    pairs = ((land.at[0], og), (land.at[1], ou), (scl.at[0], sg), (scl.at[1], su), (rt, out))
    for i, (source, target) in enumerate(pairs):
        if i < 2:
            for e in range(source.shape[0]):
                pltpu.make_async_copy(source.at[e], target.at[e], sem.at[i]).start()
        else:
            pltpu.make_async_copy(source, target, sem.at[i]).start()
    for i, (source, target) in enumerate(pairs):
        pltpu.make_async_copy(source, target, sem.at[i]).wait()


def solution(mesh):
    nz, nb = mesh.shape["zero"], mesh.shape["bank"]

    def on_device(w_gate, avg_gate, w_up, avg_up, mix_share, router_weight, router_gain):
        experts, rows, columns = w_gate.shape
        cb = columns // nz
        eb = router_weight.shape[1]
        nh = nz // 2
        head = min(HEAD, experts - 1)
        stat = (2 * (experts - head) // 8 + 1) * 8
        anyspace = pl.BlockSpec(memory_space=pl.ANY)
        vmem = pl.BlockSpec(memory_space=pltpu.VMEM)
        dma = pltpu.SemaphoreType.DMA
        flat = rows % 128 == 0
        router = (eb * nb, rows * nz) if flat else (nz, eb * nb, rows)
        f32, bf16 = jnp.float32, jnp.bfloat16
        landed = pl.pallas_call(
            functools.partial(kernel, nz, nb, head),
            out_shape=(
                pltpu.VMEM((2, experts, rows * nz, cb), bf16),
                pltpu.VMEM((2, experts, cb), f32),
                pltpu.VMEM(router, bf16),
            ),
            in_specs=[anyspace] * 7,
            out_specs=(vmem, vmem, vmem),
            scratch_shapes=[
                pltpu.SMEM((experts,), f32),
                pltpu.VMEM((eb, rows), f32),
                pltpu.VMEM((1, rows), f32),
                pltpu.VMEM((head + RING, 2, 2, rows, columns), f32),
                pltpu.VMEM((2, nz, experts, rows, cb), bf16),
                pltpu.VMEM((head, 2, nz, cb), f32),
                pltpu.VMEM((head, nz - 1, 2, nz, cb), f32),
                pltpu.VMEM((head, 2, nz, cb), f32),
                pltpu.VMEM((2, nh, stat, cb), f32),
                pltpu.VMEM((nh - 1, 2, stat, cb), f32),
                pltpu.VMEM((2, stat, cb), f32),
                pltpu.VMEM((2, stat, cb), f32),
                pltpu.VMEM((2, nh, stat, cb), f32),
                pltpu.VMEM((eb, rows), bf16),
                dma((3,)),
                dma((head + RING,)),
                dma((head,)),
                dma((head,)),
                dma((3,)),
                dma((3,)),
                dma,
                dma,
                dma((3,)),
                dma((3,)),
            ],
            compiler_params=pltpu.CompilerParams(
                collective_id=0, has_side_effects=True, vmem_limit_bytes=41_000_000
            ),
        )(mix_share, w_gate, avg_gate, w_up, avg_up, router_weight.T, router_gain[None, :])
        out = jax.ShapeDtypeStruct((experts, rows * nz, cb), bf16)
        scale = jax.ShapeDtypeStruct((experts, cb), f32)
        sg, su, cg, cu, rt = pl.pallas_call(
            settle,
            out_shape=(out, out, scale, scale, jax.ShapeDtypeStruct(router, bf16)),
            in_specs=[vmem] * 3,
            out_specs=(anyspace,) * 5,
            scratch_shapes=[dma((5,))],
            compiler_params=pltpu.CompilerParams(vmem_limit_bytes=4_000_000),
        )(*landed)
        rt = rt.T if flat else rt.transpose(0, 2, 1).reshape(nz * rows, nb * eb)
        return sg, su, cg, cu, rt

    whole = P("bank", "zero", None)
    served = P("bank", None, "zero")
    in_specs = (whole, whole, whole, whole, P("bank"), P("zero", "bank"), P("zero"))
    out_specs = (served, served, P("bank", "zero"), P("bank", "zero"), P())
    return jax.shard_map(
        on_device, mesh=mesh, in_specs=in_specs, out_specs=out_specs, check_vma=False
    )
```

```python
import functools

import jax
import jax.numpy as jnp
from jax import lax
from jax.experimental import pallas as pl
from jax.experimental.pallas import tpu as pltpu
from jax.sharding import PartitionSpec as P

MESH = pl.DeviceIdType.MESH
HEAD = 3
RING = 2
STEP = 32


def partner(me, k, n):
    out, bit = me, 1
    while bit < n:
        if k & bit:
            out = out + bit * (1 - 2 * ((me // bit) % 2))
        bit *= 2
    return out


def kernel(
    nz, nb, head,
    mix_in, wg, ag, wu, au, rw_in, gain_in,
    land, scl, rt,
    mix, rw, gain, stage, send, pa, ra, sa, part, rs, half, other, sb, rtp, raw, came,
    small_sem, in_sem, pa_ssem, pa_rsem, step_ssem, step_rsem, bulk_ssem, bulk_rsem, r_ssem, r_rsem,
):
    me = lax.axis_index("zero")
    bank = lax.axis_index("bank")
    experts, rows, _ = wg.shape
    cb = land.shape[3]
    eb = rw.shape[0]
    tail = experts - head
    nh = nz // 2
    near = lax.rem(me, nh)
    ws, avgs = (wg, wu), (ag, au)
    peers = [partner(me, k, nz) for k in range(1, nz)]
    inner, far = peers[:nh - 1], peers[nh - 1]
    banks = [partner(bank, k, nb) for k in range(1, nb)]

    early = came.shape[0]

    def loads(e, slot):
        for m in range(2):
            for i, source in enumerate((ws[m], avgs[m])):
                pltpu.make_async_copy(source.at[e], stage.at[slot, m, i], in_sem.at[slot, m]).start()

    def loaded(slot, m):
        pltpu.make_async_copy(stage.at[slot, m], stage.at[slot, m], in_sem.at[slot, m]).wait()

    def to(p, source, target, ssem, rsem):
        pltpu.make_async_remote_copy(
            source, target, ssem, rsem, device_id={"zero": p}, device_id_type=MESH).start()

    def sent(ref, sem):
        pltpu.make_async_copy(ref, ref, sem).wait()

    small = [
        pltpu.make_async_copy(mix_in, mix, small_sem.at[0]),
        pltpu.make_async_copy(rw_in, rw, small_sem.at[1]),
        pltpu.make_async_copy(gain_in, gain, small_sem.at[2]),
    ]
    small[0].start()
    loads(0, 0)

    barrier = pltpu.get_barrier_semaphore()
    for p in peers:
        pl.semaphore_signal(barrier, inc=1, device_id={"zero": p}, device_id_type=MESH)
    for p in banks:
        pl.semaphore_signal(barrier, inc=1, device_id={"bank": p}, device_id_type=MESH)
    for c in small[1:]:
        c.start()

    def ring(i):
        return head + lax.rem(i, RING)

    def fresh(slot, e, m, d, span):
        cols = slice(d * cb, (d + 1) * cb)
        a = mix[e]
        return a * stage[slot, m, 0, span, cols] + (1.0 - a) * stage[slot, m, 1, span, cols]

    def sizes_of(slot, e, m):
        def body(i, sums):
            span = pl.ds(pl.multiple_of(i * STEP, STEP), STEP)
            out = []
            for d in range(nz):
                v = jnp.abs(fresh(slot, e, m, d, span))
                out.append(sums[d] + sum(v[j:j + 8] for j in range(0, STEP, 8)))
            return tuple(out)

        sums = lax.fori_loop(0, rows // STEP, body, tuple(jnp.zeros((8, cb), jnp.float32) for _ in range(nz)))
        return [jnp.sum(s, axis=0, keepdims=True) for s in sums]

    def sizes_to_part(slot, e, row, step):
        for m in range(2):
            loaded(slot, m)
            for d, size in enumerate(sizes_of(slot, e, m)):
                part[d // nh, d % nh, pl.ds(row + m * step, 1), :] = size

    place = pl.ds(pl.multiple_of(me * rows, rows), rows)

    def narrow(slot, e, m, scale):
        inverses = [1.0 / scale(m, d) for d in range(nz)]

        def body(i, carry):
            span = pl.ds(pl.multiple_of(i * STEP, STEP), STEP)
            for d in range(nz):
                send[m, d, e, span, :] = (fresh(slot, e, m, d, span) * inverses[d]).astype(send.dtype)
            return carry

        lax.fori_loop(0, rows // STEP, body, 0)

    def push(e, m, group=2):
        land[m, e, place, :] = send[m, me, e]
        for p in peers:
            to(p, send.at[m, p, e], land.at[m, e, place], bulk_ssem.at[group], bulk_rsem.at[group])

    def push_part(i):
        span = pl.ds(i * early, early)
        target = pl.ds(pl.multiple_of(me * rows + i * early, early), early)
        land[0, 0, target, :] = send[0, me, 0, span, :]
        for k, p in enumerate(peers):
            if i or k != bound:
                to(p, send.at[0, p, 0, span], land.at[0, 0, target], bulk_ssem.at[i + 3], bulk_rsem.at[i + 3])

    def tail_sizes(i, carry):
        e = head + i
        sizes_to_part(ring(i), e, 8 + i, tail)

        @pl.when(i + RING < tail)
        def _():
            loads(e + RING, ring(i))

        return carry

    spans = (pl.ds(0, 8), pl.ds(8, part.shape[2] - 8))

    def step_in(g):
        for k, p in enumerate(inner):
            to(p, part.at[:, lax.rem(p, nh), spans[g]], rs.at[k, :, spans[g]], step_ssem.at[g, 0], step_rsem.at[g, 0])

    def step_far(g):
        sent(rs.at[:, :, spans[g]], step_rsem.at[g, 0])
        total = part[:, near, spans[g], :]
        for k in range(nh - 1):
            total = total + rs[k, :, spans[g], :]
        half[:, spans[g], :] = total
        to(far, half.at[:, spans[g]], other.at[:, spans[g]], step_ssem.at[g, 1], step_rsem.at[g, 1])

    def step_out(g):
        sent(other.at[:, spans[g]], step_rsem.at[g, 1])
        sb[:, near, spans[g], :] = (half[:, spans[g], :] + other[:, spans[g], :]) / (rows * nz)
        for m in range(2):
            if g == 0:
                scl[m, 1:head, :] = sb[me // nh, near, m * (head - 1):(m + 1) * (head - 1), :]
            else:
                scl[m, head:, :] = sb[me // nh, near, 8 + m * tail:8 + (m + 1) * tail, :]
        for p in inner:
            to(p, sb.at[:, near, spans[g]], sb.at[:, near, spans[g]], step_ssem.at[g, 2], step_rsem.at[g, 2])

    def step_done(g):
        sent(rs.at[:, :, spans[g]], step_rsem.at[g, 2])

    bound = max(nz - 3, 0)

    small[0].wait()
    loaded(0, 0)
    for e in range(1, head):
        loads(e, e)
    for i in range(min(RING, tail)):
        loads(head + i, ring(i))

    def head_send(m):
        for d, size in enumerate(sizes_of(0, 0, m)):
            pa[m, d:d + 1, :] = size
        if m == 0:
            pl.semaphore_wait(barrier, nz - 1 + nb - 1)
        for k, p in enumerate(peers):
            to(p, pa.at[m], ra.at[k, m], pa_ssem.at[m], pa_rsem.at[m])

    def head_scale(m):
        sent(ra.at[:, m], pa_rsem.at[m])
        total = pa[m]
        for k in range(nz - 1):
            total = total + ra[k, m]
        sa[m] = total / (rows * nz)
        scl[m, 0:1, :] = sa[m, pl.ds(me, 1), :]

    def keep(i, carry):
        span = pl.ds(pl.multiple_of(i * 16, 16), 16)
        for d in range(nz):
            raw[d, span, :] = fresh(0, 0, 0, d, span)
        return carry

    head_send(0)
    lax.fori_loop(0, early // 16, keep, 0)
    to(peers[bound], raw.at[peers[bound]], came, bulk_ssem.at[1], bulk_rsem.at[1])
    loaded(0, 1)
    head_send(1)
    part[...] = jnp.zeros_like(part)
    for e in range(1, head):
        sizes_to_part(e, e, e - 1, head - 1)
    step_in(0)
    for c in small[1:]:
        c.wait()
    rtp[...] = (rw[...] * gain[...]).astype(rtp.dtype)
    band = pl.ds(pl.multiple_of(bank * eb, eb), eb)
    flat = len(rt.shape) == 2
    if flat:
        mine = rt.at[band, place]
        theirs = rt.at[band, pl.ds(pl.multiple_of(far * rows, rows), rows)]
        tiles = rt.at[band, pl.ds(0, 2 * (nh - 1) * rows)]
        column = rt.at[band]
        others = rt.at[pl.ds(0, (nb - 1) * eb)]
        rt[band, place] = rtp[...]
    else:
        mine = rt.at[me, band]
        theirs = rt.at[far, band]
        tiles = rt.at[pl.ds(0, 2 * (nh - 1)), band]
        column = rt.at[:, band]
        others = rt.at[:, pl.ds(0, (nb - 1) * eb)]
        rt[me, band] = rtp[...]

    head_scale(0)
    narrow(0, 0, 0, lambda m, d: sa[m, d:d + 1, :])
    push_part(0)
    step_far(0)
    push_part(1)
    head_scale(1)
    narrow(0, 0, 1, lambda m, d: sa[m, d:d + 1, :])
    to(far, rtp, mine, r_ssem.at[0], r_rsem.at[0])

    def serve_head(e, m):
        narrow(e, e, m, lambda m, d: sb[d // nh, d % nh, pl.ds(m * (head - 1) + e - 1, 1), :])
        push(e, m)

    lax.fori_loop(0, tail // 3, tail_sizes, 0)
    step_out(0)
    push(0, 1, 0)
    lax.fori_loop(tail // 3, 2 * tail // 3, tail_sizes, 0)
    step_done(0)
    serve_head(1, 0)
    lax.fori_loop(2 * tail // 3, tail, tail_sizes, 0)
    step_in(1)
    for i in range(min(RING, tail)):
        loads(head + i, ring(i))
    serve_head(1, 1)
    step_far(1)
    serve_head(2, 0)
    step_out(1)
    pltpu.make_async_copy(theirs, theirs, r_rsem.at[0]).wait()
    for p in inner:
        for tile in (mine, theirs):
            to(p, tile, tile, r_ssem.at[1], r_rsem.at[1])
    serve_head(2, 1)

    sent(tiles, r_rsem.at[1])
    for p in banks:
        pltpu.make_async_remote_copy(
            column, column, r_ssem.at[2], r_rsem.at[2], device_id={"bank": p}, device_id_type=MESH).start()
    step_done(1)

    def serve(i, carry):
        e = head + i
        for m in range(2):
            loaded(ring(i), m)
            narrow(ring(i), e, m, lambda m, d: sb[d // nh, d % nh, pl.ds(8 + m * tail + i, 1), :])
            push(e, m)

        @pl.when(i + RING < tail)
        def _():
            loads(e + RING, ring(i))

        return carry

    lax.fori_loop(0, tail, serve, 0)

    sent(came, bulk_rsem.at[1])
    inverse = 1.0 / sa[0, pl.ds(me, 1), :]

    def widen(i, carry):
        span = pl.ds(pl.multiple_of(i * 16, 16), 16)
        rest = pl.ds(pl.multiple_of(peers[bound] * rows + i * 16, 16), 16)
        land[0, 0, rest, :] = (came[span, :] * inverse).astype(land.dtype)
        return carry

    lax.fori_loop(0, early // 16, widen, 0)
    sent(came, bulk_ssem.at[1])
    for m in range(2):
        sent(ra.at[:, m], pa_ssem.at[m])
    for g in range(2):
        sent(rs.at[:, :, spans[g]], step_ssem.at[g, 0])
        sent(other.at[:, spans[g]], step_ssem.at[g, 1])
        sent(rs.at[:, :, spans[g]], step_ssem.at[g, 2])
    sent(rtp, r_ssem.at[0])
    sent(tiles, r_ssem.at[1])
    for sem in (r_ssem, r_rsem):
        sent(others, sem.at[2])
    for sems in (bulk_ssem, bulk_rsem):
        sent(land.at[1, 0, pl.ds(0, (nz - 1) * rows)], sems.at[0])
        sent(land.at[:, pl.ds(1, experts - 1), pl.ds(0, (nz - 1) * rows)], sems.at[2])
        sent(land.at[0, 0, pl.ds(0, (nz - 2) * early)], sems.at[3])
        sent(land.at[0, 0, pl.ds(0, (nz - 1) * early)], sems.at[4])


def settle(land, scl, rt, og, ou, sg, su, out, sem):
    pairs = ((land.at[0], og), (land.at[1], ou), (scl.at[0], sg), (scl.at[1], su), (rt, out))
    for i, (source, target) in enumerate(pairs):
        if i < 2:
            for e in range(source.shape[0]):
                pltpu.make_async_copy(source.at[e], target.at[e], sem.at[i]).start()
        else:
            pltpu.make_async_copy(source, target, sem.at[i]).start()
    for i, (source, target) in enumerate(pairs):
        pltpu.make_async_copy(source, target, sem.at[i]).wait()


def solution(mesh):
    nz, nb = mesh.shape["zero"], mesh.shape["bank"]

    def on_device(w_gate, avg_gate, w_up, avg_up, mix_share, router_weight, router_gain):
        experts, rows, columns = w_gate.shape
        cb = columns // nz
        eb = router_weight.shape[1]
        nh = nz // 2
        head = min(HEAD, experts)
        stat = 8 + (2 * (experts - head) // 8 + 1) * 8
        early = rows // 2
        anyspace = pl.BlockSpec(memory_space=pl.ANY)
        vmem = pl.BlockSpec(memory_space=pltpu.VMEM)
        dma = pltpu.SemaphoreType.DMA
        flat = rows % 128 == 0
        router = (eb * nb, rows * nz) if flat else (nz, eb * nb, rows)
        f32, bf16 = jnp.float32, jnp.bfloat16
        landed = pl.pallas_call(
            functools.partial(kernel, nz, nb, head),
            out_shape=(
                pltpu.VMEM((2, experts, rows * nz, cb), bf16),
                pltpu.VMEM((2, experts, cb), f32),
                pltpu.VMEM(router, bf16),
            ),
            in_specs=[anyspace] * 7,
            out_specs=(vmem, vmem, vmem),
            scratch_shapes=[
                pltpu.SMEM((experts,), f32),
                pltpu.VMEM((eb, rows), f32),
                pltpu.VMEM((1, rows), f32),
                pltpu.VMEM((head + RING, 2, 2, rows, columns), f32),
                pltpu.VMEM((2, nz, experts, rows, cb), bf16),
                pltpu.VMEM((2, nz, cb), f32),
                pltpu.VMEM((nz - 1, 2, nz, cb), f32),
                pltpu.VMEM((2, nz, cb), f32),
                pltpu.VMEM((2, nh, stat, cb), f32),
                pltpu.VMEM((nh - 1, 2, stat, cb), f32),
                pltpu.VMEM((2, stat, cb), f32),
                pltpu.VMEM((2, stat, cb), f32),
                pltpu.VMEM((2, nh, stat, cb), f32),
                pltpu.VMEM((eb, rows), bf16),
                pltpu.VMEM((nz, early, cb), f32),
                pltpu.VMEM((early, cb), f32),
                dma((3,)),
                dma((head + RING, 2)),
                dma((2,)),
                dma((2,)),
                dma((2, 3)),
                dma((2, 3)),
                dma((5,)),
                dma((5,)),
                dma((3,)),
                dma((3,)),
            ],
            compiler_params=pltpu.CompilerParams(
                collective_id=0, has_side_effects=True, vmem_limit_bytes=44_000_000
            ),
        )(mix_share, w_gate, avg_gate, w_up, avg_up, router_weight.T, router_gain[None, :])
        out = jax.ShapeDtypeStruct((experts, rows * nz, cb), bf16)
        scale = jax.ShapeDtypeStruct((experts, cb), f32)
        sg, su, cg, cu, rt = pl.pallas_call(
            settle,
            out_shape=(out, out, scale, scale, jax.ShapeDtypeStruct(router, bf16)),
            in_specs=[vmem] * 3,
            out_specs=(anyspace,) * 5,
            scratch_shapes=[dma((5,))],
            compiler_params=pltpu.CompilerParams(vmem_limit_bytes=4_000_000),
        )(*landed)
        rt = rt.T if flat else rt.transpose(0, 2, 1).reshape(nz * rows, nb * eb)
        return sg, su, cg, cu, rt

    whole = P("bank", "zero", None)
    served = P("bank", None, "zero")
    in_specs = (whole, whole, whole, whole, P("bank"), P("zero", "bank"), P("zero"))
    out_specs = (served, served, P("bank", "zero"), P("bank", "zero"), P())
    return jax.shard_map(
        on_device, mesh=mesh, in_specs=in_specs, out_specs=out_specs, check_vma=False
    )
```

```python
import functools

import jax
import jax.numpy as jnp
from jax import lax
from jax.experimental import pallas as pl
from jax.experimental.pallas import tpu as pltpu
from jax.sharding import PartitionSpec as P

MESH = pl.DeviceIdType.MESH
HEAD = 3
RING = 2
STEP = 32


def partner(me, k, n):
    out, bit = me, 1
    while bit < n:
        if k & bit:
            out = out + bit * (1 - 2 * ((me // bit) % 2))
        bit *= 2
    return out


def kernel(
    nz, nb, head,
    mix_in, wg, ag, wu, au, rw_in, gain_in,
    land, scl, rt,
    mix, rw, gain, stage, send, pa, ra, sa, part, rs, half, other, sb, rtp, raw, came,
    small_sem, in_sem, pa_ssem, pa_rsem, step_ssem, step_rsem, bulk_ssem, bulk_rsem, r_ssem, r_rsem,
):
    me = lax.axis_index("zero")
    bank = lax.axis_index("bank")
    experts, rows, _ = wg.shape
    cb = land.shape[3]
    eb = rw.shape[0]
    tail = experts - head
    nh = nz // 2
    near = lax.rem(me, nh)
    ws, avgs = (wg, wu), (ag, au)
    peers = [partner(me, k, nz) for k in range(1, nz)]
    inner, far = peers[:nh - 1], peers[nh - 1]
    banks = [partner(bank, k, nb) for k in range(1, nb)]

    early = came.shape[0]

    def loads(e, slot):
        for m in range(2):
            for i, source in enumerate((ws[m], avgs[m])):
                pltpu.make_async_copy(source.at[e], stage.at[slot, m, i], in_sem.at[slot, m]).start()

    def loaded(slot, m):
        pltpu.make_async_copy(stage.at[slot, m], stage.at[slot, m], in_sem.at[slot, m]).wait()

    def to(p, source, target, ssem, rsem):
        pltpu.make_async_remote_copy(
            source, target, ssem, rsem, device_id={"zero": p}, device_id_type=MESH).start()

    def sent(ref, sem):
        pltpu.make_async_copy(ref, ref, sem).wait()

    small = [
        pltpu.make_async_copy(mix_in, mix, small_sem.at[0]),
        pltpu.make_async_copy(rw_in, rw, small_sem.at[1]),
        pltpu.make_async_copy(gain_in, gain, small_sem.at[2]),
    ]
    small[0].start()
    loads(0, 0)

    barrier = pltpu.get_barrier_semaphore()
    for p in peers:
        pl.semaphore_signal(barrier, inc=1, device_id={"zero": p}, device_id_type=MESH)
    for p in banks:
        pl.semaphore_signal(barrier, inc=1, device_id={"bank": p}, device_id_type=MESH)
    for c in small[1:]:
        c.start()

    def ring(i):
        return head + lax.rem(i, RING)

    def fresh(slot, e, m, d, span):
        cols = slice(d * cb, (d + 1) * cb)
        a = mix[e]
        return a * stage[slot, m, 0, span, cols] + (1.0 - a) * stage[slot, m, 1, span, cols]

    def sizes_of(slot, e, m):
        def body(i, sums):
            span = pl.ds(pl.multiple_of(i * STEP, STEP), STEP)
            out = []
            for d in range(nz):
                v = jnp.abs(fresh(slot, e, m, d, span))
                out.append(sums[d] + sum(v[j:j + 8] for j in range(0, STEP, 8)))
            return tuple(out)

        sums = lax.fori_loop(0, rows // STEP, body, tuple(jnp.zeros((8, cb), jnp.float32) for _ in range(nz)))
        return [jnp.sum(s, axis=0, keepdims=True) for s in sums]

    def sizes_to_part(slot, e, row, step):
        for m in range(2):
            loaded(slot, m)
            for d, size in enumerate(sizes_of(slot, e, m)):
                part[d // nh, d % nh, pl.ds(row + m * step, 1), :] = size

    place = pl.ds(pl.multiple_of(me * rows, rows), rows)

    def narrow(slot, e, m, scale):
        inverses = [1.0 / scale(m, d) for d in range(nz)]

        def body(i, carry):
            span = pl.ds(pl.multiple_of(i * STEP, STEP), STEP)
            for d in range(nz):
                send[m, d, e, span, :] = (fresh(slot, e, m, d, span) * inverses[d]).astype(send.dtype)
            return carry

        lax.fori_loop(0, rows // STEP, body, 0)

    def push(e, m, group=2):
        land[m, e, place, :] = send[m, me, e]
        for p in peers:
            to(p, send.at[m, p, e], land.at[m, e, place], bulk_ssem.at[group], bulk_rsem.at[group])

    def push_part(i):
        lo, n = (early, rows - early) if i else (0, early)
        span = pl.ds(lo, n)
        target = pl.ds(pl.multiple_of(me * rows + lo, 16), n)
        land[0, 0, target, :] = send[0, me, 0, span, :]
        for k, p in enumerate(peers):
            if i or k != bound:
                to(p, send.at[0, p, 0, span], land.at[0, 0, target], bulk_ssem.at[i + 3], bulk_rsem.at[i + 3])

    def tail_sizes(i, carry):
        e = head + i
        sizes_to_part(ring(i), e, 8 + i, tail)

        @pl.when(i + RING < tail)
        def _():
            loads(e + RING, ring(i))

        return carry

    spans = (pl.ds(0, 8), pl.ds(8, part.shape[2] - 8))

    def step_in(g):
        for k, p in enumerate(inner):
            to(p, part.at[:, lax.rem(p, nh), spans[g]], rs.at[k, :, spans[g]], step_ssem.at[g, 0], step_rsem.at[g, 0])

    def step_far(g):
        sent(rs.at[:, :, spans[g]], step_rsem.at[g, 0])
        total = part[:, near, spans[g], :]
        for k in range(nh - 1):
            total = total + rs[k, :, spans[g], :]
        half[:, spans[g], :] = total
        to(far, half.at[:, spans[g]], other.at[:, spans[g]], step_ssem.at[g, 1], step_rsem.at[g, 1])

    def step_out(g):
        sent(other.at[:, spans[g]], step_rsem.at[g, 1])
        sb[:, near, spans[g], :] = (half[:, spans[g], :] + other[:, spans[g], :]) / (rows * nz)
        for m in range(2):
            if g == 0:
                scl[m, 1:head, :] = sb[me // nh, near, m * (head - 1):(m + 1) * (head - 1), :]
            else:
                scl[m, head:, :] = sb[me // nh, near, 8 + m * tail:8 + (m + 1) * tail, :]
        for p in inner:
            to(p, sb.at[:, near, spans[g]], sb.at[:, near, spans[g]], step_ssem.at[g, 2], step_rsem.at[g, 2])

    def step_done(g):
        sent(rs.at[:, :, spans[g]], step_rsem.at[g, 2])

    bound = max(nz - 3, 0)

    small[0].wait()
    loaded(0, 0)
    for e in range(1, head):
        loads(e, e)
    for i in range(min(RING, tail)):
        loads(head + i, ring(i))

    def head_send(m):
        for d, size in enumerate(sizes_of(0, 0, m)):
            pa[m, d:d + 1, :] = size
        if m == 0:
            pl.semaphore_wait(barrier, nz - 1 + nb - 1)
        for k, p in enumerate(peers):
            to(p, pa.at[m], ra.at[k, m], pa_ssem.at[m], pa_rsem.at[m])

    def head_scale(m):
        sent(ra.at[:, m], pa_rsem.at[m])
        total = pa[m]
        for k in range(nz - 1):
            total = total + ra[k, m]
        sa[m] = total / (rows * nz)
        scl[m, 0:1, :] = sa[m, pl.ds(me, 1), :]

    def keep(i, carry):
        span = pl.ds(pl.multiple_of(i * 16, 16), 16)
        for d in range(nz):
            raw[d, span, :] = fresh(0, 0, 0, d, span)
        return carry

    head_send(0)
    lax.fori_loop(0, early // 16, keep, 0)
    to(peers[bound], raw.at[peers[bound]], came, bulk_ssem.at[1], bulk_rsem.at[1])
    loaded(0, 1)
    head_send(1)
    part[...] = jnp.zeros_like(part)
    for e in range(1, head):
        sizes_to_part(e, e, e - 1, head - 1)
    step_in(0)
    for c in small[1:]:
        c.wait()
    rtp[...] = (rw[...] * gain[...]).astype(rtp.dtype)
    band = pl.ds(pl.multiple_of(bank * eb, eb), eb)
    flat = len(rt.shape) == 2
    if flat:
        mine = rt.at[band, place]
        theirs = rt.at[band, pl.ds(pl.multiple_of(far * rows, rows), rows)]
        tiles = rt.at[band, pl.ds(0, 2 * (nh - 1) * rows)]
        column = rt.at[band]
        others = rt.at[pl.ds(0, (nb - 1) * eb)]
        rt[band, place] = rtp[...]
    else:
        mine = rt.at[me, band]
        theirs = rt.at[far, band]
        tiles = rt.at[pl.ds(0, 2 * (nh - 1)), band]
        column = rt.at[:, band]
        others = rt.at[:, pl.ds(0, (nb - 1) * eb)]
        rt[me, band] = rtp[...]

    head_scale(0)
    narrow(0, 0, 0, lambda m, d: sa[m, d:d + 1, :])
    push_part(0)
    step_far(0)
    push_part(1)
    head_scale(1)
    narrow(0, 0, 1, lambda m, d: sa[m, d:d + 1, :])
    to(far, rtp, mine, r_ssem.at[0], r_rsem.at[0])

    def serve_head(e, m):
        narrow(e, e, m, lambda m, d: sb[d // nh, d % nh, pl.ds(m * (head - 1) + e - 1, 1), :])
        push(e, m)

    lax.fori_loop(0, tail // 3, tail_sizes, 0)
    step_out(0)
    push(0, 1, 0)
    lax.fori_loop(tail // 3, 2 * tail // 3, tail_sizes, 0)
    step_done(0)
    serve_head(1, 0)
    lax.fori_loop(2 * tail // 3, tail, tail_sizes, 0)
    step_in(1)
    for i in range(min(RING, tail)):
        loads(head + i, ring(i))
    serve_head(1, 1)
    step_far(1)
    serve_head(2, 0)
    step_out(1)
    pltpu.make_async_copy(theirs, theirs, r_rsem.at[0]).wait()
    for p in inner:
        for tile in (mine, theirs):
            to(p, tile, tile, r_ssem.at[1], r_rsem.at[1])
    serve_head(2, 1)

    sent(tiles, r_rsem.at[1])
    for p in banks:
        pltpu.make_async_remote_copy(
            column, column, r_ssem.at[2], r_rsem.at[2], device_id={"bank": p}, device_id_type=MESH).start()
    step_done(1)

    def serve(i, carry):
        e = head + i
        for m in range(2):
            loaded(ring(i), m)
            narrow(ring(i), e, m, lambda m, d: sb[d // nh, d % nh, pl.ds(8 + m * tail + i, 1), :])
            push(e, m)

        @pl.when(i + RING < tail)
        def _():
            loads(e + RING, ring(i))

        return carry

    lax.fori_loop(0, tail - 1, serve, 0)
    e = experts - 1
    for m in range(2):
        loaded(ring(tail - 1), m)
        narrow(ring(tail - 1), e, m, lambda m, d: sb[d // nh, d % nh, pl.ds(8 + (m + 1) * tail - 1, 1), :])
        land[m, e, place, :] = send[m, me, e]
    for p in peers:
        for m in range(2):
            to(p, send.at[m, p, e], land.at[m, e, place], bulk_ssem.at[2], bulk_rsem.at[2])

    sent(came, bulk_rsem.at[1])
    inverse = 1.0 / sa[0, pl.ds(me, 1), :]

    def widen(i, carry):
        span = pl.ds(pl.multiple_of(i * 16, 16), 16)
        rest = pl.ds(pl.multiple_of(peers[bound] * rows + i * 16, 16), 16)
        land[0, 0, rest, :] = (came[span, :] * inverse).astype(land.dtype)
        return carry

    lax.fori_loop(0, early // 16, widen, 0)
    sent(came, bulk_ssem.at[1])
    for m in range(2):
        sent(ra.at[:, m], pa_ssem.at[m])
    for g in range(2):
        sent(rs.at[:, :, spans[g]], step_ssem.at[g, 0])
        sent(other.at[:, spans[g]], step_ssem.at[g, 1])
        sent(rs.at[:, :, spans[g]], step_ssem.at[g, 2])
    sent(rtp, r_ssem.at[0])
    sent(tiles, r_ssem.at[1])
    for sem in (r_ssem, r_rsem):
        sent(others, sem.at[2])
    for sems in (bulk_ssem, bulk_rsem):
        sent(land.at[1, 0, pl.ds(0, (nz - 1) * rows)], sems.at[0])
        sent(land.at[:, pl.ds(1, experts - 1), pl.ds(0, (nz - 1) * rows)], sems.at[2])
        sent(land.at[0, 0, pl.ds(0, (nz - 2) * early)], sems.at[3])
        sent(land.at[0, 0, pl.ds(0, (nz - 1) * (rows - early))], sems.at[4])


def settle(land, scl, rt, og, ou, sg, su, out, sem):
    pairs = ((land.at[0], og), (land.at[1], ou), (scl.at[0], sg), (scl.at[1], su), (rt, out))
    for i, (source, target) in enumerate(pairs):
        if i < 2:
            for e in range(source.shape[0]):
                pltpu.make_async_copy(source.at[e], target.at[e], sem.at[i]).start()
        else:
            pltpu.make_async_copy(source, target, sem.at[i]).start()
    for i, (source, target) in enumerate(pairs):
        pltpu.make_async_copy(source, target, sem.at[i]).wait()


def solution(mesh):
    nz, nb = mesh.shape["zero"], mesh.shape["bank"]

    def on_device(w_gate, avg_gate, w_up, avg_up, mix_share, router_weight, router_gain):
        experts, rows, columns = w_gate.shape
        cb = columns // nz
        eb = router_weight.shape[1]
        nh = nz // 2
        head = min(HEAD, experts)
        stat = 8 + (2 * (experts - head) // 8 + 1) * 8
        early = rows * 3 // 4 // 16 * 16
        anyspace = pl.BlockSpec(memory_space=pl.ANY)
        vmem = pl.BlockSpec(memory_space=pltpu.VMEM)
        dma = pltpu.SemaphoreType.DMA
        flat = rows % 128 == 0
        router = (eb * nb, rows * nz) if flat else (nz, eb * nb, rows)
        f32, bf16 = jnp.float32, jnp.bfloat16
        landed = pl.pallas_call(
            functools.partial(kernel, nz, nb, head),
            out_shape=(
                pltpu.VMEM((2, experts, rows * nz, cb), bf16),
                pltpu.VMEM((2, experts, cb), f32),
                pltpu.VMEM(router, bf16),
            ),
            in_specs=[anyspace] * 7,
            out_specs=(vmem, vmem, vmem),
            scratch_shapes=[
                pltpu.SMEM((experts,), f32),
                pltpu.VMEM((eb, rows), f32),
                pltpu.VMEM((1, rows), f32),
                pltpu.VMEM((head + RING, 2, 2, rows, columns), f32),
                pltpu.VMEM((2, nz, experts, rows, cb), bf16),
                pltpu.VMEM((2, nz, cb), f32),
                pltpu.VMEM((nz - 1, 2, nz, cb), f32),
                pltpu.VMEM((2, nz, cb), f32),
                pltpu.VMEM((2, nh, stat, cb), f32),
                pltpu.VMEM((nh - 1, 2, stat, cb), f32),
                pltpu.VMEM((2, stat, cb), f32),
                pltpu.VMEM((2, stat, cb), f32),
                pltpu.VMEM((2, nh, stat, cb), f32),
                pltpu.VMEM((eb, rows), bf16),
                pltpu.VMEM((nz, early, cb), f32),
                pltpu.VMEM((early, cb), f32),
                dma((3,)),
                dma((head + RING, 2)),
                dma((2,)),
                dma((2,)),
                dma((2, 3)),
                dma((2, 3)),
                dma((5,)),
                dma((5,)),
                dma((3,)),
                dma((3,)),
            ],
            compiler_params=pltpu.CompilerParams(
                collective_id=0, has_side_effects=True, vmem_limit_bytes=44_000_000
            ),
        )(mix_share, w_gate, avg_gate, w_up, avg_up, router_weight.T, router_gain[None, :])
        out = jax.ShapeDtypeStruct((experts, rows * nz, cb), bf16)
        scale = jax.ShapeDtypeStruct((experts, cb), f32)
        sg, su, cg, cu, rt = pl.pallas_call(
            settle,
            out_shape=(out, out, scale, scale, jax.ShapeDtypeStruct(router, bf16)),
            in_specs=[vmem] * 3,
            out_specs=(anyspace,) * 5,
            scratch_shapes=[dma((5,))],
            compiler_params=pltpu.CompilerParams(vmem_limit_bytes=4_000_000),
        )(*landed)
        rt = rt.T if flat else rt.transpose(0, 2, 1).reshape(nz * rows, nb * eb)
        return sg, su, cg, cu, rt

    whole = P("bank", "zero", None)
    served = P("bank", None, "zero")
    in_specs = (whole, whole, whole, whole, P("bank"), P("zero", "bank"), P("zero"))
    out_specs = (served, served, P("bank", "zero"), P("bank", "zero"), P())
    return jax.shard_map(
        on_device, mesh=mesh, in_specs=in_specs, out_specs=out_specs, check_vma=False
    )
```

```python
import functools

import jax
import jax.numpy as jnp
from jax import lax
from jax.experimental import pallas as pl
from jax.experimental.pallas import tpu as pltpu
from jax.sharding import PartitionSpec as P

MESH = pl.DeviceIdType.MESH
HEAD = 3
RING = 2
STEP = 32


def partner(me, k, n):
    out, bit = me, 1
    while bit < n:
        if k & bit:
            out = out + bit * (1 - 2 * ((me // bit) % 2))
        bit *= 2
    return out


def kernel(
    nz, nb, head,
    mix_in, wg, ag, wu, au, rw_in, gain_in,
    land, scl, rt,
    mix, rw, gain, stage, send, pa, ra, sa, part, rs, half, other, sb, rtp, raw, came,
    small_sem, in_sem, pa_ssem, pa_rsem, step_ssem, step_rsem, bulk_ssem, bulk_rsem, r_ssem, r_rsem,
):
    me = lax.axis_index("zero")
    bank = lax.axis_index("bank")
    experts, rows, _ = wg.shape
    cb = land.shape[3]
    eb = rw.shape[0]
    tail = experts - head
    nh = nz // 2
    near = lax.rem(me, nh)
    ws, avgs = (wg, wu), (ag, au)
    peers = [partner(me, k, nz) for k in range(1, nz)]
    inner, far = peers[:nh - 1], peers[nh - 1]
    banks = [partner(bank, k, nb) for k in range(1, nb)]

    early = came.shape[0]

    def loads(e, slot):
        for m in range(2):
            for i, source in enumerate((ws[m], avgs[m])):
                pltpu.make_async_copy(source.at[e], stage.at[slot, m, i], in_sem.at[slot, m]).start()

    def loaded(slot, m):
        pltpu.make_async_copy(stage.at[slot, m], stage.at[slot, m], in_sem.at[slot, m]).wait()

    def to(p, source, target, ssem, rsem):
        pltpu.make_async_remote_copy(
            source, target, ssem, rsem, device_id={"zero": p}, device_id_type=MESH).start()

    def sent(ref, sem):
        pltpu.make_async_copy(ref, ref, sem).wait()

    small = [
        pltpu.make_async_copy(mix_in, mix, small_sem.at[0]),
        pltpu.make_async_copy(rw_in, rw, small_sem.at[1]),
        pltpu.make_async_copy(gain_in, gain, small_sem.at[2]),
    ]
    small[0].start()
    loads(0, 0)

    barrier = pltpu.get_barrier_semaphore()
    for p in peers:
        pl.semaphore_signal(barrier, inc=1, device_id={"zero": p}, device_id_type=MESH)
    for p in banks:
        pl.semaphore_signal(barrier, inc=1, device_id={"bank": p}, device_id_type=MESH)
    for c in small[1:]:
        c.start()

    def ring(i):
        return head + lax.rem(i, RING)

    def fresh(slot, e, m, d, span):
        cols = slice(d * cb, (d + 1) * cb)
        a = mix[e]
        return a * stage[slot, m, 0, span, cols] + (1.0 - a) * stage[slot, m, 1, span, cols]

    def sizes_of(slot, e, m):
        def body(i, sums):
            span = pl.ds(pl.multiple_of(i * STEP, STEP), STEP)
            out = []
            for d in range(nz):
                v = jnp.abs(fresh(slot, e, m, d, span))
                out.append(sums[d] + sum(v[j:j + 8] for j in range(0, STEP, 8)))
            return tuple(out)

        sums = lax.fori_loop(0, rows // STEP, body, tuple(jnp.zeros((8, cb), jnp.float32) for _ in range(nz)))
        return [jnp.sum(s, axis=0, keepdims=True) for s in sums]

    def sizes_to_part(slot, e, row, step):
        for m in range(2):
            loaded(slot, m)
            for d, size in enumerate(sizes_of(slot, e, m)):
                part[d // nh, d % nh, pl.ds(row + m * step, 1), :] = size

    place = pl.ds(pl.multiple_of(me * rows, rows), rows)

    def narrow(slot, e, m, scale, lo=0, hi=None):
        inverses = [1.0 / scale(m, d) for d in range(nz)]

        def body(i, carry):
            span = pl.ds(pl.multiple_of(i * STEP, STEP), STEP)
            for d in range(nz):
                send[m, d, e, span, :] = (fresh(slot, e, m, d, span) * inverses[d]).astype(send.dtype)
            return carry

        lax.fori_loop(lo, rows // STEP if hi is None else hi, body, 0)

    def push(e, m, group=2):
        land[m, e, place, :] = send[m, me, e]
        for p in peers:
            to(p, send.at[m, p, e], land.at[m, e, place], bulk_ssem.at[group], bulk_rsem.at[group])

    def push_part(i):
        lo, n = (early, rows - early) if i else (0, early)
        span = pl.ds(lo, n)
        target = pl.ds(pl.multiple_of(me * rows + lo, 16), n)
        land[0, 0, target, :] = send[0, me, 0, span, :]
        for k, p in enumerate(peers):
            if i or k != bound:
                to(p, send.at[0, p, 0, span], land.at[0, 0, target], bulk_ssem.at[i + 3], bulk_rsem.at[i + 3])

    def tail_sizes(i, carry):
        e = head + i
        sizes_to_part(ring(i), e, 8 + i, tail)

        @pl.when(i + RING < tail)
        def _():
            loads(e + RING, ring(i))

        return carry

    spans = (pl.ds(0, 8), pl.ds(8, part.shape[2] - 8))

    def step_in(g):
        for k, p in enumerate(inner):
            to(p, part.at[:, lax.rem(p, nh), spans[g]], rs.at[k, :, spans[g]], step_ssem.at[g, 0], step_rsem.at[g, 0])

    def step_far(g):
        sent(rs.at[:, :, spans[g]], step_rsem.at[g, 0])
        total = part[:, near, spans[g], :]
        for k in range(nh - 1):
            total = total + rs[k, :, spans[g], :]
        half[:, spans[g], :] = total
        to(far, half.at[:, spans[g]], other.at[:, spans[g]], step_ssem.at[g, 1], step_rsem.at[g, 1])

    def step_out(g):
        sent(other.at[:, spans[g]], step_rsem.at[g, 1])
        sb[:, near, spans[g], :] = (half[:, spans[g], :] + other[:, spans[g], :]) / (rows * nz)
        for m in range(2):
            if g == 0:
                scl[m, 1:head, :] = sb[me // nh, near, m * (head - 1):(m + 1) * (head - 1), :]
            else:
                scl[m, head:, :] = sb[me // nh, near, 8 + m * tail:8 + (m + 1) * tail, :]
        for p in inner:
            to(p, sb.at[:, near, spans[g]], sb.at[:, near, spans[g]], step_ssem.at[g, 2], step_rsem.at[g, 2])

    def step_done(g):
        sent(rs.at[:, :, spans[g]], step_rsem.at[g, 2])

    bound = max(nz - 3, 0)

    small[0].wait()
    loaded(0, 0)
    for e in range(1, head):
        loads(e, e)
    for i in range(min(RING, tail)):
        loads(head + i, ring(i))

    def head_send(m):
        for d, size in enumerate(sizes_of(0, 0, m)):
            pa[m, d:d + 1, :] = size
        if m == 0:
            pl.semaphore_wait(barrier, nz - 1 + nb - 1)
        for k, p in enumerate(peers):
            to(p, pa.at[m], ra.at[k, m], pa_ssem.at[m], pa_rsem.at[m])

    def head_scale(m):
        sent(ra.at[:, m], pa_rsem.at[m])
        total = pa[m]
        for k in range(nz - 1):
            total = total + ra[k, m]
        sa[m] = total / (rows * nz)
        scl[m, 0:1, :] = sa[m, pl.ds(me, 1), :]

    def keep(i, carry):
        span = pl.ds(pl.multiple_of(i * 16, 16), 16)
        for d in range(nz):
            raw[d, span, :] = fresh(0, 0, 0, d, span)
        return carry

    head_send(0)
    lax.fori_loop(0, early // 16, keep, 0)
    to(peers[bound], raw.at[peers[bound]], came, bulk_ssem.at[1], bulk_rsem.at[1])
    loaded(0, 1)
    head_send(1)
    part[...] = jnp.zeros_like(part)
    for e in range(1, head):
        sizes_to_part(e, e, e - 1, head - 1)
    step_in(0)
    for c in small[1:]:
        c.wait()
    rtp[...] = (rw[...] * gain[...]).astype(rtp.dtype)
    band = pl.ds(pl.multiple_of(bank * eb, eb), eb)
    flat = len(rt.shape) == 2
    if flat:
        mine = rt.at[band, place]
        theirs = rt.at[band, pl.ds(pl.multiple_of(far * rows, rows), rows)]
        tiles = rt.at[band, pl.ds(0, 2 * (nh - 1) * rows)]
        column = rt.at[band]
        others = rt.at[pl.ds(0, (nb - 1) * eb)]
        rt[band, place] = rtp[...]
    else:
        mine = rt.at[me, band]
        theirs = rt.at[far, band]
        tiles = rt.at[pl.ds(0, 2 * (nh - 1)), band]
        column = rt.at[:, band]
        others = rt.at[:, pl.ds(0, (nb - 1) * eb)]
        rt[me, band] = rtp[...]

    head_scale(0)
    cut = -(-early // STEP)
    narrow(0, 0, 0, lambda m, d: sa[m, d:d + 1, :], 0, cut)
    push_part(0)
    narrow(0, 0, 0, lambda m, d: sa[m, d:d + 1, :], cut)
    step_far(0)
    push_part(1)
    head_scale(1)
    narrow(0, 0, 1, lambda m, d: sa[m, d:d + 1, :])
    to(far, rtp, mine, r_ssem.at[0], r_rsem.at[0])

    def serve_head(e, m):
        narrow(e, e, m, lambda m, d: sb[d // nh, d % nh, pl.ds(m * (head - 1) + e - 1, 1), :])
        push(e, m)

    lax.fori_loop(0, tail // 3, tail_sizes, 0)
    step_out(0)
    push(0, 1, 0)
    lax.fori_loop(tail // 3, 2 * tail // 3, tail_sizes, 0)
    step_done(0)
    serve_head(1, 0)
    lax.fori_loop(2 * tail // 3, tail, tail_sizes, 0)
    step_in(1)
    for i in range(min(RING, tail)):
        loads(head + i, ring(i))
    serve_head(1, 1)
    step_far(1)
    serve_head(2, 0)
    step_out(1)
    pltpu.make_async_copy(theirs, theirs, r_rsem.at[0]).wait()
    for p in inner:
        for tile in (mine, theirs):
            to(p, tile, tile, r_ssem.at[1], r_rsem.at[1])
    serve_head(2, 1)

    sent(tiles, r_rsem.at[1])
    for p in banks:
        pltpu.make_async_remote_copy(
            column, column, r_ssem.at[2], r_rsem.at[2], device_id={"bank": p}, device_id_type=MESH).start()
    step_done(1)

    def serve(i, carry):
        e = head + i
        for m in range(2):
            loaded(ring(i), m)
            narrow(ring(i), e, m, lambda m, d: sb[d // nh, d % nh, pl.ds(8 + m * tail + i, 1), :])
            push(e, m)

        @pl.when(i + RING < tail)
        def _():
            loads(e + RING, ring(i))

        return carry

    lax.fori_loop(0, tail - 1, serve, 0)
    e = experts - 1
    for m in range(2):
        loaded(ring(tail - 1), m)
        narrow(ring(tail - 1), e, m, lambda m, d: sb[d // nh, d % nh, pl.ds(8 + (m + 1) * tail - 1, 1), :])
        land[m, e, place, :] = send[m, me, e]
    for p in peers:
        for m in range(2):
            to(p, send.at[m, p, e], land.at[m, e, place], bulk_ssem.at[2], bulk_rsem.at[2])

    sent(came, bulk_rsem.at[1])
    inverse = 1.0 / sa[0, pl.ds(me, 1), :]

    def widen(i, carry):
        span = pl.ds(pl.multiple_of(i * 16, 16), 16)
        rest = pl.ds(pl.multiple_of(peers[bound] * rows + i * 16, 16), 16)
        land[0, 0, rest, :] = (came[span, :] * inverse).astype(land.dtype)
        return carry

    lax.fori_loop(0, early // 16, widen, 0)
    sent(came, bulk_ssem.at[1])
    for m in range(2):
        sent(ra.at[:, m], pa_ssem.at[m])
    for g in range(2):
        sent(rs.at[:, :, spans[g]], step_ssem.at[g, 0])
        sent(other.at[:, spans[g]], step_ssem.at[g, 1])
        sent(rs.at[:, :, spans[g]], step_ssem.at[g, 2])
    sent(rtp, r_ssem.at[0])
    sent(tiles, r_ssem.at[1])
    for sem in (r_ssem, r_rsem):
        sent(others, sem.at[2])
    for sems in (bulk_ssem, bulk_rsem):
        sent(land.at[1, 0, pl.ds(0, (nz - 1) * rows)], sems.at[0])
        sent(land.at[:, pl.ds(1, experts - 1), pl.ds(0, (nz - 1) * rows)], sems.at[2])
        sent(land.at[0, 0, pl.ds(0, (nz - 2) * early)], sems.at[3])
        sent(land.at[0, 0, pl.ds(0, (nz - 1) * (rows - early))], sems.at[4])


def settle(land, scl, rt, og, ou, sg, su, out, sem):
    pairs = ((land.at[0], og), (land.at[1], ou), (scl.at[0], sg), (scl.at[1], su), (rt, out))
    for i, (source, target) in enumerate(pairs):
        if i < 2:
            for e in range(source.shape[0]):
                pltpu.make_async_copy(source.at[e], target.at[e], sem.at[i]).start()
        else:
            pltpu.make_async_copy(source, target, sem.at[i]).start()
    for i, (source, target) in enumerate(pairs):
        pltpu.make_async_copy(source, target, sem.at[i]).wait()


def solution(mesh):
    nz, nb = mesh.shape["zero"], mesh.shape["bank"]

    def on_device(w_gate, avg_gate, w_up, avg_up, mix_share, router_weight, router_gain):
        experts, rows, columns = w_gate.shape
        cb = columns // nz
        eb = router_weight.shape[1]
        nh = nz // 2
        head = min(HEAD, experts)
        stat = 8 + 2 * (experts - head)
        early = rows * 3 // 4 // 16 * 16
        anyspace = pl.BlockSpec(memory_space=pl.ANY)
        vmem = pl.BlockSpec(memory_space=pltpu.VMEM)
        dma = pltpu.SemaphoreType.DMA
        flat = rows % 128 == 0
        router = (eb * nb, rows * nz) if flat else (nz, eb * nb, rows)
        f32, bf16 = jnp.float32, jnp.bfloat16
        landed = pl.pallas_call(
            functools.partial(kernel, nz, nb, head),
            out_shape=(
                pltpu.VMEM((2, experts, rows * nz, cb), bf16),
                pltpu.VMEM((2, experts, cb), f32),
                pltpu.VMEM(router, bf16),
            ),
            in_specs=[anyspace] * 7,
            out_specs=(vmem, vmem, vmem),
            scratch_shapes=[
                pltpu.SMEM((experts,), f32),
                pltpu.VMEM((eb, rows), f32),
                pltpu.VMEM((1, rows), f32),
                pltpu.VMEM((head + RING, 2, 2, rows, columns), f32),
                pltpu.VMEM((2, nz, experts, rows, cb), bf16),
                pltpu.VMEM((2, nz, cb), f32),
                pltpu.VMEM((nz - 1, 2, nz, cb), f32),
                pltpu.VMEM((2, nz, cb), f32),
                pltpu.VMEM((2, nh, stat, cb), f32),
                pltpu.VMEM((nh - 1, 2, stat, cb), f32),
                pltpu.VMEM((2, stat, cb), f32),
                pltpu.VMEM((2, stat, cb), f32),
                pltpu.VMEM((2, nh, stat, cb), f32),
                pltpu.VMEM((eb, rows), bf16),
                pltpu.VMEM((nz, early, cb), f32),
                pltpu.VMEM((early, cb), f32),
                dma((3,)),
                dma((head + RING, 2)),
                dma((2,)),
                dma((2,)),
                dma((2, 3)),
                dma((2, 3)),
                dma((5,)),
                dma((5,)),
                dma((3,)),
                dma((3,)),
            ],
            compiler_params=pltpu.CompilerParams(
                collective_id=0, has_side_effects=True, vmem_limit_bytes=44_000_000
            ),
        )(mix_share, w_gate, avg_gate, w_up, avg_up, router_weight.T, router_gain[None, :])
        out = jax.ShapeDtypeStruct((experts, rows * nz, cb), bf16)
        scale = jax.ShapeDtypeStruct((experts, cb), f32)
        sg, su, cg, cu, rt = pl.pallas_call(
            settle,
            out_shape=(out, out, scale, scale, jax.ShapeDtypeStruct(router, bf16)),
            in_specs=[vmem] * 3,
            out_specs=(anyspace,) * 5,
            scratch_shapes=[dma((5,))],
            compiler_params=pltpu.CompilerParams(vmem_limit_bytes=4_000_000),
        )(*landed)
        rt = rt.T if flat else rt.transpose(0, 2, 1).reshape(nz * rows, nb * eb)
        return sg, su, cg, cu, rt

    whole = P("bank", "zero", None)
    served = P("bank", None, "zero")
    in_specs = (whole, whole, whole, whole, P("bank"), P("zero", "bank"), P("zero"))
    out_specs = (served, served, P("bank", "zero"), P("bank", "zero"), P())
    return jax.shard_map(
        on_device, mesh=mesh, in_specs=in_specs, out_specs=out_specs, check_vma=False
    )
```
